128 devices in a mesh: expert: 8 (over y_hi, x), shard: 16 (over z, y_lo, core).
Axes of the slice: x: 4, y: 4 (y_hi: 2, y_lo: 2; y = y_hi * 2 + y_lo), z: 4, core: 2. Of those that a mesh axis runs over, the one named last changes fastest.
Arguments:
- tokens: bfloat16 [1024, 4096], P(('expert', 'shard')), may hold values from -6 to 6
- cotangent: bfloat16 [1024, 4096], P(('expert', 'shard')), may hold values from -6 to 6
- expert_ids: int32 [1024, 2], P(('expert', 'shard')), may hold values from 0 to 7, as said below
- slot_ids: int32 [1024, 2], P(('expert', 'shard')), may hold values from 0 to 3, as said below
- route_weight: float32 [1024, 2], P(('expert', 'shard')), may hold values from 0.1 to 1
- w_gate: bfloat16 [8, 4096, 7168], P('expert', 'shard'), may hold values from -0.09375 to 0.09375
- w_up: bfloat16 [8, 4096, 7168], P('expert', 'shard'), may hold values from -0.09375 to 0.09375
- w_down: bfloat16 [8, 4096, 7168], P('expert', 'shard'), may hold values from -0.0625 to 0.0625
Outputs:
- layer_out: bfloat16 [1024, 4096], P(('expert', 'shard'))
- d_tokens: bfloat16 [1024, 4096], P(('expert', 'shard'))
- grad_gate: bfloat16 [8, 4096, 7168], P('expert', 'shard')
- grad_up: bfloat16 [8, 4096, 7168], P('expert', 'shard')
- grad_down: bfloat16 [8, 4096, 7168], P('expert', 'shard')
The draws below stay inside these ranges and needn't reach their ends.
Inputs may be any that keep to these rules, and one draw needn't show every extreme that they name: `expert_ids`: A token's two ids differ. Among the 8 tokens of one block no expert is named more than 4 times, and in every draw, for each index along shard, one expert is named exactly 4 times in each of the 8 blocks that share that index. Assignment k of a token takes slot slot_ids[., k] of the expert expert_ids[., k]; the assignments of one block to one expert have distinct slots.
All inputs are finite; a program needn't handle non-finite values.
Results may differ from the reference program's by a relative error of at most 0.019.
Values may be sent and summed in bfloat16 or wider, within the bound.
No kernel may reach another device: no remote copies, remote signals or barrier semaphores. Data moves between devices by JAX's collectives and lax.ppermute only.
A program may use at most 128 MiB of HBM per device.

```python
import jax
import jax.numpy as jnp
from jax import lax

D = 4096
FFW = 7168
TOK_DEV = 8
EXPERTS = 8
SHARDS = 16
BLOCKS = 128
TOKENS = 1024
CAP = 4
ROWS = 512


def route_tables(key):
    base_key = jax.random.fold_in(key, 1234)
    key_hot, key_bias, key_noise, key_order, key_swap = jax.random.split(base_key, 5)
    cell_count = EXPERTS * CAP
    hot_shard = jax.random.randint(key_hot, (SHARDS,), 0, EXPERTS)
    hot_block = jnp.tile(hot_shard, BLOCKS // SHARDS)
    expert_bias = jax.random.randint(key_bias, (BLOCKS, EXPERTS), 0, 4)
    noise = jax.random.randint(key_noise, (BLOCKS, cell_count), 0, 65536)
    cell_ids = jnp.arange(cell_count, dtype=jnp.int32)
    cell_expert = cell_ids // CAP
    boost = (cell_expert[None, :] == hot_block[:, None]).astype(jnp.int32) * 2 ** 28
    scores = (noise + expert_bias[:, cell_expert] * 65536) * cell_count + cell_ids[None, :] + boost
    chosen = lax.top_k(scores, 2 * TOK_DEV)[1]
    chosen = jnp.sort(chosen, axis=1)
    paired = jnp.stack([chosen[:, :TOK_DEV], chosen[:, TOK_DEV:]], axis=-1)
    order_keys = jax.random.randint(key_order, (BLOCKS, TOK_DEV), 0, 65536) * TOK_DEV + jnp.arange(TOK_DEV, dtype=jnp.int32)[None, :]
    order = jnp.argsort(order_keys, axis=1)
    paired = jnp.take_along_axis(paired, order[:, :, None], axis=1)
    swapped = jax.random.randint(key_swap, (BLOCKS, TOK_DEV, 1), 0, 2)
    paired = jnp.where(swapped == 1, paired[:, :, ::-1], paired)
    paired = paired.reshape(BLOCKS * TOK_DEV, 2).astype(jnp.int32)
    return (paired // CAP, paired % CAP)


def draw_expert_ids(key, part):
    return route_tables(key)[0]


def draw_slot_ids(key, part):
    return route_tables(key)[1]


def block_levels(key, dims, cuts, low, high):
    def one(dim, shards_of):
        heights = jax.random.uniform(jax.random.fold_in(jax.random.fold_in(key, 6), dim), (shards_of,), jnp.float32, low / len(cuts), high / len(cuts))
        return jnp.repeat(jnp.exp(heights), dims[dim] // shards_of).reshape((-1,) + (1,) * (len(dims) - dim - 1))

    level = one(*cuts[0])
    for cut in cuts[1:]:
        level = level * one(*cut)
    return level


def centred(rng, dims, scale, bound, shards=(), kind=jnp.bfloat16):
    drawn = scale * jax.random.normal(rng, dims, jnp.float32)
    if shards:
        drawn = drawn * block_levels(rng, dims, shards, -0.22, 0.18)
    return jnp.clip(drawn, -bound, bound).astype(kind)


def setup_inputs(seed: int = 0) -> dict:
    streams_of = jax.random.split(jax.random.key(seed), 9)
    return {
        "tokens": centred(streams_of[0], (TOKENS, D), 1.0, 6.0, ((0, 128),)),
        "cotangent": centred(streams_of[1], (TOKENS, D), 1.0, 6.0, ((0, 128),)),
        "expert_ids": draw_expert_ids(jax.random.fold_in(streams_of[8], 71), 0),
        "slot_ids": draw_slot_ids(jax.random.fold_in(streams_of[8], 71), 0),
        "route_weight": jnp.clip(0.1 + 0.9 * jax.random.uniform(streams_of[4], (TOKENS, 2), jnp.float32) ** block_levels(streams_of[4], (TOKENS, 2), ((0, 128),), -0.2, 0.2), 0.1, 1.0),
        "w_gate": centred(streams_of[5], (EXPERTS, D, FFW), D ** -0.5, 0.09375, ((0, 8), (1, 16))),
        "w_up": centred(streams_of[6], (EXPERTS, D, FFW), D ** -0.5, 0.09375, ((0, 8), (1, 16))),
        "w_down": centred(streams_of[7], (EXPERTS, D, FFW), FFW ** -0.5, 0.0625, ((0, 8), (1, 16))),
    }


def silu_parts(gate_value):
    logistic = jax.nn.sigmoid(gate_value)
    return gate_value * logistic, logistic * (1.0 + gate_value * (1.0 - logistic))


def grouped_sum(pairs):
    row_count = pairs[0][0].shape[0]
    width = FFW // SHARDS
    partials = jnp.zeros((SHARDS, row_count, D), jnp.float32)
    for left_side, right_side in pairs:
        left_group = left_side.astype(jnp.float32).reshape(row_count, SHARDS, width)
        right_group = right_side.astype(jnp.float32).reshape(D, SHARDS, width)
        partials = partials + jnp.einsum("rsf,dsf->srd", left_group, right_group, precision=lax.Precision.HIGHEST)
    rounded = lax.optimization_barrier(partials.astype(jnp.bfloat16)).astype(jnp.float32)
    return jnp.sum(rounded, axis=0)


def expert_pass(group_rows, d_rows, gate_matrix, up_matrix, down_matrix):
    gate_value = jnp.dot(group_rows, gate_matrix, preferred_element_type=jnp.float32)
    up_value = jnp.dot(group_rows, up_matrix, preferred_element_type=jnp.float32)
    activation, silu_slope = silu_parts(gate_value)
    hidden = (activation * up_value).astype(jnp.bfloat16)
    expert_out = grouped_sum([(hidden, down_matrix)]).astype(jnp.bfloat16)
    d_hidden = jnp.dot(d_rows, down_matrix, preferred_element_type=jnp.float32)
    grad_down = jnp.dot(d_rows.T, hidden, preferred_element_type=jnp.float32).astype(jnp.bfloat16)
    d_gate = (d_hidden * up_value * silu_slope).astype(jnp.bfloat16)
    d_up = (d_hidden * activation).astype(jnp.bfloat16)
    grad_gate = jnp.dot(group_rows.T, d_gate, preferred_element_type=jnp.float32).astype(jnp.bfloat16)
    grad_up = jnp.dot(group_rows.T, d_up, preferred_element_type=jnp.float32).astype(jnp.bfloat16)
    d_expert = grouped_sum([(d_gate, gate_matrix), (d_up, up_matrix)]).astype(jnp.bfloat16)
    return expert_out, d_expert, grad_gate, grad_up, grad_down


def by_expert(slot_rows):
    shaped = slot_rows.reshape(BLOCKS, EXPERTS, CAP, D)
    return jnp.transpose(shaped, (1, 0, 2, 3)).reshape(EXPERTS, ROWS, D)


def by_block(expert_rows):
    shaped = expert_rows.reshape(EXPERTS, BLOCKS, CAP, D)
    return jnp.transpose(shaped, (1, 0, 2, 3)).reshape(BLOCKS, EXPERTS * CAP, D).astype(jnp.float32)


def reference(tokens, cotangent, expert_ids, slot_ids, route_weight, w_gate, w_up, w_down):
    slot_index = expert_ids * CAP + slot_ids
    columns = jnp.arange(EXPERTS * CAP, dtype=jnp.int32)
    slot_match = (slot_index[:, :, None] == columns[None, None, :]).astype(jnp.float32)
    dispatch = jnp.sum(slot_match, axis=1).reshape(BLOCKS, TOK_DEV, EXPERTS * CAP)
    combine = jnp.sum(slot_match * route_weight[:, :, None], axis=1).reshape(BLOCKS, TOK_DEV, EXPERTS * CAP)
    token_blocks = tokens.astype(jnp.float32).reshape(BLOCKS, TOK_DEV, D)
    cotangent_blocks = cotangent.astype(jnp.float32).reshape(BLOCKS, TOK_DEV, D)
    x_slots = jnp.einsum("btc,btd->bcd", dispatch, token_blocks, precision=lax.Precision.HIGHEST).astype(jnp.bfloat16)
    d_slots = jnp.einsum("btc,btd->bcd", combine, cotangent_blocks, precision=lax.Precision.HIGHEST).astype(jnp.bfloat16)
    results = lax.map(lambda inputs: expert_pass(*inputs), (by_expert(x_slots), by_expert(d_slots), w_gate, w_up, w_down))
    expert_out, d_expert, grad_gate, grad_up, grad_down = results
    layer_out = jnp.einsum("btc,bcd->btd", combine, by_block(expert_out), precision=lax.Precision.HIGHEST)
    d_tokens = jnp.einsum("btc,bcd->btd", dispatch, by_block(d_expert), precision=lax.Precision.HIGHEST)
    layer_out = layer_out.reshape(TOKENS, D).astype(jnp.bfloat16)
    d_tokens = d_tokens.reshape(TOKENS, D).astype(jnp.bfloat16)
    return layer_out, d_tokens, grad_gate, grad_up, grad_down
```

```python
import functools

import jax
import jax.numpy as jnp
from jax import lax
from jax.experimental import pallas as pl
from jax.experimental.pallas import tpu as pltpu
from jax.sharding import PartitionSpec as P

CAP = 4
BLK = 32
TRI = 3 * BLK
TN = 512
CHUNKS = (("Z", 4096), ("Y", 3072))
BF = jnp.bfloat16
F32 = jnp.float32


def hop(dz, dy, dc):
    pairs = []
    for z in range(4):
        for y in range(2):
            for c in range(2):
                pairs.append((z * 4 + y * 2 + c, ((z + dz) % 4) * 4 + (y ^ dy) * 2 + (c ^ dc)))
    return pairs


def up_z(v):
    return lax.ppermute(v, "shard", hop(1, 0, 0))


def down_z(v):
    return lax.ppermute(v, "shard", hop(3, 0, 0))


def swap_y(v):
    return lax.ppermute(v, "shard", hop(0, 1, 0))


def swap_core(v):
    return lax.ppermute(v, "shard", hop(0, 0, 1))


def dot(a, b):
    return jnp.dot(a, b, preferred_element_type=F32)


def dot_t(a, b):
    return lax.dot_general(a, b, (((1,), (1,)), ((), ())), preferred_element_type=F32)


def cost(flops, nbytes):
    return pl.CostEstimate(flops=int(flops), bytes_accessed=int(nbytes), transcendentals=0)


PLACE = {
    "Z": {
        (2, 0): (0, 0),
        (2, 1): (1, 0),
        (1, 0): (2, 0),
        (1, 1): (2, 1),
        (3, 0): (3, 0),
        (3, 1): (3, 1),
        (0, 0): (4, 0),
        (0, 1): (4, 1),
    },
    "Y": {(dz, dy): (1 - dy, dz) for dz in range(4) for dy in range(2)},
}
SIZES = {"Z": (1, 1, 2, 2, 2), "Y": (4, 4)}


def partial_kernel(kind, x0, x1, g0, u0, d0, g1, u1, d1, *outs):
    half = x0.shape[1] // 2
    xa, xb = x0[:, :half], x1[:, :half]
    da, db = x0[:, half:], x1[:, half:]
    values = (
        dot(xa, g0[0]) + dot(xb, g1[0]),
        dot(xa, u0[0]) + dot(xb, u1[0]),
        dot(da, d0[0]) + dot(db, d1[0]),
    )
    for k, value in enumerate(values):
        rounded = value.astype(BF)
        for (dz, dy), (which, place) in PLACE[kind].items():
            block = dz * 2 + dy
            row = place * TRI + k * BLK
            outs[which][row : row + BLK, :] = rounded[block * BLK : (block + 1) * BLK, :]


def partial_sums(kind, first, width, x0, x1, own, partner):
    off = first // TN
    rows, depth = own[0].shape[1], x0.shape[0]
    wspec = pl.BlockSpec((1, rows, TN), lambda j: (0, 0, j + off))
    xspec = pl.BlockSpec(x0.shape, lambda j: (0, 0))
    sizes = SIZES[kind]
    return pl.pallas_call(
        functools.partial(partial_kernel, kind),
        grid=(width // TN,),
        in_specs=[xspec, xspec] + [wspec] * 6,
        out_specs=[pl.BlockSpec((n * TRI, TN), lambda j: (0, j)) for n in sizes],
        out_shape=[jax.ShapeDtypeStruct((n * TRI, width), BF) for n in sizes],
        cost_estimate=cost(2 * 6 * depth * rows * width, 2 * width * (6 * rows + 3 * depth)),
        name="partial_sums",
    )(x0, x1, *own, *partner)


def rowwise(name, body, inputs, outs, width, alias=None):
    tile = width // 2 if width <= 2048 else width // 4
    in_specs = [pl.BlockSpec((n, tile), functools.partial(lambda i, j: (i, j), i)) for _, i, n in inputs]

    def kernel(*refs):
        ins, results = refs[: len(inputs)], refs[len(inputs) :]
        for ref, value in zip(results, body([r[...] for r in ins]), strict=True):
            ref[...] = value

    moved = sum(n for _, _, n in inputs) + sum(n for n, _, _ in outs)
    return pl.pallas_call(
        kernel,
        grid=(width // tile,),
        in_specs=in_specs,
        out_specs=[pl.BlockSpec((n, tile), functools.partial(lambda i, j: (i, j), i)) for n, i, _ in outs],
        out_shape=[jax.ShapeDtypeStruct((full, width), BF) for _, _, full in outs],
        input_output_aliases=alias or {},
        cost_estimate=cost(64 * moved * width, 2 * moved * width),
        name=name,
    )(*[a for a, _, _ in inputs])


def f32_sum(values):
    total = values[0].astype(F32)
    for v in values[1:]:
        total = total + v.astype(F32)
    return total


def activate(total):
    gate, up, d_hidden = total[:BLK], total[BLK : 2 * BLK], total[2 * BLK :]
    logistic = 1.0 / (1.0 + jnp.exp(-gate))
    activation = gate * logistic
    slope = logistic * (1.0 + gate * (1.0 - logistic))
    return jnp.concatenate([activation * up, d_hidden * up * slope, d_hidden * activation], axis=0).astype(BF)


def scatter_z(parts, width):
    far_a, far_b, plus, minus, own = parts
    got_a, got_b = up_z(far_a), down_z(far_b)
    plus, minus = rowwise(
        "add_far",
        lambda v: [f32_sum(v[:2]).astype(BF), f32_sum(v[2:]).astype(BF)],
        [(plus, 0, TRI), (got_a, 0, TRI), (minus, 1, TRI), (got_b, 0, TRI)],
        [(TRI, 0, 2 * TRI), (TRI, 1, 2 * TRI)],
        width,
        {0: 0, 2: 1},
    )
    from_minus, from_plus = up_z(plus), down_z(minus)
    (send,) = rowwise(
        "add_near",
        lambda v: [f32_sum(v).astype(BF)],
        [(own, 1, TRI), (from_minus, 1, TRI), (from_plus, 1, TRI)],
        [(TRI, 0, TRI)],
        width,
    )
    got_y = swap_y(send)
    (mine,) = rowwise(
        "activate",
        lambda v: [activate(f32_sum(v))],
        [(own, 0, TRI), (from_minus, 0, TRI), (from_plus, 0, TRI), (got_y, 0, TRI)],
        [(TRI, 0, TRI)],
        width,
    )
    return mine


def gather_y_z(mine):
    pair = jnp.concatenate([mine, swap_y(mine)], axis=0)
    from_minus, from_plus = up_z(pair), down_z(pair)
    far_a, far_b = up_z(from_minus[:TRI]), down_z(from_plus[TRI:])
    chip = jnp.concatenate([pair, from_plus, far_a, far_b, from_minus], axis=0)
    return [chip, swap_core(chip)]


def scatter_y(parts, width):
    send, own = parts
    got_y = swap_y(send)
    half = TRI // 2
    far_a, far_b = rowwise(
        "add_y",
        lambda v: [f32_sum(v[:2]).astype(BF), f32_sum(v[2:]).astype(BF)],
        [(own, 4, half), (got_y, 4, half), (own, 5, half), (got_y, 5, half)],
        [(half, 0, half), (half, 0, half)],
        width,
    )
    got_a, got_b = up_z(far_a), down_z(far_b)

    def near(v):
        plus = f32_sum(v[:2])
        minus = f32_sum(v[2:4])
        plus = jnp.concatenate([plus[:half] + v[4].astype(F32), plus[half:]], axis=0)
        minus = jnp.concatenate([minus[:half], minus[half:] + v[5].astype(F32)], axis=0)
        return [plus.astype(BF), minus.astype(BF)]

    plus, minus = rowwise(
        "add_far",
        near,
        [(own, 1, TRI), (got_y, 1, TRI), (own, 3, TRI), (got_y, 3, TRI), (got_a, 0, half), (got_b, 0, half)],
        [(TRI, 0, TRI), (TRI, 0, TRI)],
        width,
    )
    from_minus, from_plus = up_z(plus), down_z(minus)
    (mine,) = rowwise(
        "activate",
        lambda v: [activate(f32_sum(v))],
        [(own, 0, TRI), (got_y, 0, TRI), (from_minus, 0, TRI), (from_plus, 0, TRI)],
        [(TRI, 0, TRI)],
        width,
    )
    return mine


def gather_z_y(mine):
    half = TRI // 2
    from_minus, from_plus = up_z(mine), down_z(mine)
    far_a, far_b = up_z(from_minus[:half]), down_z(from_plus[half:])
    column = jnp.concatenate([mine, from_plus, far_a, far_b, from_minus], axis=0)
    other = swap_y(column)
    return [column, other, swap_core(column), swap_core(other)]


def block_at(kind, dc, dz, dy):
    if kind == "Z":
        return dc, (dz * 2 + dy) * TRI
    return dc * 2 + dy, dz * TRI


def final_kernel(kind, n_in, *refs):
    pieces = refs[:n_in]
    xt, gate, up, down = refs[n_in : n_in + 4]
    grad_gate, grad_up, grad_down, out, d_out = refs[-5:]
    order = [block_at(kind, dc, dz, dy) for dc in range(2) for dz in range(4) for dy in range(2)]

    def rows(k):
        return jnp.concatenate([pieces[w][r + k * BLK : r + (k + 1) * BLK, :] for w, r in order], axis=0)

    hidden, d_gate, d_up = rows(0), rows(1), rows(2)
    half = xt.shape[0] // 2
    grad_down[0] = dot(xt[half:, :], hidden).astype(BF)
    grad_gate[0] = dot(xt[:half, :], d_gate).astype(BF)
    grad_up[0] = dot(xt[:half, :], d_up).astype(BF)

    @pl.when(pl.program_id(0) == 0)
    def _():
        out[...] = jnp.zeros_like(out)
        d_out[...] = jnp.zeros_like(d_out)

    out[...] += dot_t(hidden, down[0])
    d_out[...] += dot_t(d_gate, gate[0]) + dot_t(d_up, up[0])


def final(kind, first, width, pieces, xt, own, grads):
    off = first // TN
    rows, total = own[0].shape[1:]
    n_rows = xt.shape[1]
    wspec = pl.BlockSpec((1, rows, TN), lambda j: (0, 0, j + off))
    whole = pl.BlockSpec((n_rows, rows), lambda j: (0, 0))
    in_specs = [pl.BlockSpec((p.shape[0], TN), lambda j: (0, j)) for p in pieces]
    in_specs += [pl.BlockSpec(xt.shape, lambda j: (0, 0))] + [wspec] * 3
    n_in = len(pieces)
    alias = {}
    if grads:
        in_specs += [pl.BlockSpec(memory_space=pl.ANY)] * 3
        alias = {n_in + 4 + k: k for k in range(3)}
    return pl.pallas_call(
        functools.partial(final_kernel, kind, n_in),
        grid=(width // TN,),
        in_specs=in_specs,
        out_specs=[wspec] * 3 + [whole] * 2,
        out_shape=[jax.ShapeDtypeStruct((1, rows, total), BF)] * 3 + [jax.ShapeDtypeStruct((n_rows, rows), F32)] * 2,
        input_output_aliases=alias,
        cost_estimate=cost(2 * 6 * n_rows * rows * width, 2 * width * (6 * rows + 3 * n_rows)),
        name="final",
    )(*pieces, xt, *own, *grads)


def per_device(tokens, cotangent, expert_ids, slot_ids, route_weight, w_gate, w_up, w_down):
    experts = lax.axis_size("expert")
    shards = lax.axis_size("shard")
    width = tokens.shape[1]
    part = width // shards
    hidden_units = w_gate.shape[2]
    own = (w_gate, w_up, w_down)
    partner = tuple(swap_core(w) for w in own)

    slot_index = expert_ids * CAP + slot_ids
    columns = jnp.arange(experts * CAP, dtype=jnp.int32)
    slot_match = (slot_index[:, :, None] == columns[None, None, :]).astype(F32)
    dispatch = jnp.sum(slot_match, axis=1).astype(BF)
    combine = jnp.sum(slot_match * route_weight[:, :, None], axis=1)
    x_slots = jnp.einsum("tc,td->cd", dispatch, tokens, preferred_element_type=F32).astype(BF)
    d_slots = jnp.dot(combine.T, cotangent.astype(F32)).astype(BF)

    n_rows = experts * shards * CAP
    me = lax.axis_index("shard")
    row = lax.broadcasted_iota(jnp.int32, (n_rows, n_rows), 0)
    col = lax.broadcasted_iota(jnp.int32, (n_rows, n_rows), 1)

    def source(r):
        block, inner = r // BLK, r % BLK
        dc, dz, dy = block // 8, (block // 2) % 4, block % 2
        z = (me // 4 + dz) % 4
        y = ((me // 2) % 2 + dy) % 2
        c = (me % 2 + dc) % 2
        return (inner // CAP) * (shards * CAP) + (z * 4 + y * 2 + c) * CAP + inner % CAP

    reorder = (source(row) == col).astype(BF)

    both = jnp.stack([x_slots, d_slots], axis=0).reshape(2, experts, CAP, shards, part)
    sent = jnp.transpose(both, (1, 3, 2, 0, 4)).reshape(n_rows, 2 * part)
    arrived = lax.all_to_all(sent, ("expert", "shard"), split_axis=0, concat_axis=0, tiled=True)
    x_rel = dot(reorder, arrived).astype(BF)
    xt = lax.dot_general(arrived, reorder, (((0,), (1,)), ((), ())), preferred_element_type=F32).astype(BF)
    x0 = x_rel[: n_rows // 2]
    x1 = swap_core(x_rel[n_rows // 2 :])

    scattered = []
    first = 0
    for kind, w in CHUNKS:
        scattered.append((kind, first, w, partial_sums(kind, first, w, x0, x1, own, partner)))
        first += w
    assert first == hidden_units
    grads, out, d_out = (), 0.0, 0.0
    for kind, first, w, parts in scattered:
        if kind == "Z":
            pieces = gather_y_z(scatter_z(parts, w))
        else:
            pieces = gather_z_y(scatter_y(parts, w))
        *grads, out_c, d_out_c = final(kind, first, w, pieces, xt, own, grads)
        out, d_out = out + out_c, d_out + d_out_c

    results = jnp.concatenate([out, d_out], axis=1).astype(BF)
    returned = lax.dot_general(reorder, results, (((0,), (0,)), ((), ())), preferred_element_type=F32).astype(BF)
    back = lax.all_to_all(returned, ("expert", "shard"), split_axis=0, concat_axis=0, tiled=True)
    back = back.reshape(experts, shards, CAP, 2, part)
    back = jnp.transpose(back, (3, 0, 2, 1, 4)).reshape(2, experts * CAP, width)
    layer_out = jnp.dot(combine, back[0].astype(F32)).astype(BF)
    d_tokens = jnp.dot(dispatch, back[1], preferred_element_type=F32).astype(BF)
    return (layer_out, d_tokens, *grads)


def solution(mesh):
    rows = P(("expert", "shard"), None)
    weights = P("expert", "shard", None)
    return jax.shard_map(
        per_device,
        mesh=mesh,
        in_specs=(rows,) * 5 + (weights,) * 3,
        out_specs=(rows, rows, weights, weights, weights),
        check_vma=False,
    )
```
